32 devices in a mesh: ctx: 16 (over z, y, x), tp: 2 (over core).
Axes of the slice: x: 2, y: 2, z: 4, core: 2. Of those that a mesh axis runs over, the one named last changes fastest.
Arguments:
- queries: bfloat16 [1024, 2560], P('ctx', 'tp'), may hold values from -100 to 100
- projected_keys: bfloat16 [1024, 512], P('ctx', 'tp'), may hold values from -30 to 30
- projected_values: bfloat16 [1024, 512], P('ctx', 'tp'), may hold values from -6 to 6
- hidden: bfloat16 [1024, 5120], P('ctx', 'tp'), may hold values from -6 to 6
- route_ids: int32 [1024, 1], P('ctx'), may hold values from 0 to 15; in each aligned block of 64 rows (0 to 63, 64 to 127, ...) at most 6 rows name the same one
- route_gain: float32 [1024], P('ctx'), may hold values from 0.25 to 1
- w_gate: bfloat16 [16, 5120, 4096], P('ctx', None, 'tp'), may hold values from -0.078125 to 0.078125
- w_up: bfloat16 [16, 5120, 4096], P('ctx', None, 'tp'), may hold values from -0.078125 to 0.078125
- w_down: bfloat16 [16, 4096, 5120], P('ctx', None, 'tp'), may hold values from -0.09375 to 0.09375
Outputs:
- attended: bfloat16 [1024, 2560], P('ctx', 'tp')
- mixed: bfloat16 [1024, 5120], P('ctx', 'tp')
The draws below stay inside these ranges and needn't reach their ends.
Inputs may be any that keep to these rules, and one draw needn't show every extreme that they name: `route_ids`: within the rows of one device (aligned blocks of 64 rows) no expert is named more than 6 times, a bound that some block reaches.
All inputs are finite; a program needn't handle non-finite values.
Results may differ from the reference program's by a relative error of at most 0.0057.
Values may be sent and summed in bfloat16 or wider, within the bound.
No kernel may reach another device: no remote copies, remote signals or barrier semaphores. Data moves between devices by JAX's collectives and lax.ppermute only.
A program may use at most 128 MiB of HBM per device.

```python
import math
import jax
import jax.numpy as jnp
import numpy as np
from jax import lax

D = 5120
HEAD_SIZE = 128
QUERY_HEADS = 20
KEY_VALUE_HEADS = 4
EXPERTS = 16
FF = 4096
TOK_DEV = 64
CAP = 6
SEQUENCE_TOKENS = 1024
HOSTS = 1
N_CTX = 16


def drawn_pair(key):
    key_sample = jax.random.normal(jax.random.fold_in(key, 11), (SEQUENCE_TOKENS, KEY_VALUE_HEADS * HEAD_SIZE), jnp.float32)
    query_draw = jax.random.normal(jax.random.fold_in(key, 12), (SEQUENCE_TOKENS, QUERY_HEADS * HEAD_SIZE), jnp.float32)
    return (query_draw, key_sample)


def draw_queries(key, part):
    return drawn_pair(key)[0].astype(jnp.bfloat16)


def draw_projected_keys(key, part):
    return drawn_pair(key)[1].astype(jnp.bfloat16)


def level_of(key, dims, cuts, smallest, high):
    loudness, own = 1.0, jax.random.fold_in(key, 6)
    for dim, parts in cuts:
        draws = jnp.exp(jax.random.uniform(jax.random.fold_in(own, dim), (parts,), jnp.float32, smallest / len(cuts), high / len(cuts)))
        loudness = loudness * jnp.repeat(draws, dims[dim] // parts).reshape([-1 if axis == dim else 1 for axis in range(len(dims))])
    return loudness


def routed_block(stream_key, own, number, rows, count, top, reach, lean):
    sequence = jax.random.permutation(stream_key, count)
    crowded, ordinary = shares(count, rows * top, reach, lean, True), shares(count, rows * top, reach, lean, False)
    places = jnp.arange(count)

    def named(tallies, offset_by):
        used = int((tallies > 0).sum())
        fixed = max(1, used // 4)
        moved = fixed + (places - fixed + offset_by * (used - fixed)) % max(1, count - fixed)
        return jnp.zeros((count,), jnp.int32).at[sequence[jnp.where(places < fixed, places, moved)]].set(jnp.asarray(tallies, jnp.int32))

    tallies = jnp.where(number % 4 == 0, named(crowded, number // 4), named(ordinary, number - number // 4 - 1))
    mixed = jax.random.permutation(jax.random.fold_in(own, 3), count)
    source_of, sink = mixed[0:count // 2 * 2:2], mixed[1:count // 2 * 2:2]
    slack = jnp.minimum(tallies[source_of] - 1, reach - tallies[sink]) // 2
    slack = jnp.where((source_of == sequence[0]) | (sink == sequence[0]) | (tallies[sink] == 0), 0, jnp.maximum(slack, 0))
    moved = jax.random.randint(jax.random.fold_in(own, 4), (count // 2,), 0, 1 << 20) % (slack + 1)
    tallies = tallies.at[source_of].add(-moved).at[sink].add(moved)
    items = jnp.searchsorted(jnp.cumsum(tallies), jnp.arange(rows * top), side="right").astype(jnp.int32)
    grid = items.reshape(top, rows).T
    grid = grid[jax.random.permutation(jax.random.fold_in(own, 1), rows)]
    offset_by = jax.random.randint(jax.random.fold_in(own, 2), (rows, 1), 0, top)
    return jnp.take_along_axis(grid, (jnp.arange(top)[None, :] + offset_by) % top, axis=1)


def shares(count, total, most, skew, full):
    weights = [(1 << 20) // math.isqrt(rank ** skew) + 1 for rank in range(1, count + 1)]
    largest = most if full else min(most, max(-(-total // count), total * weights[0] // sum(weights)))
    least = 1 if total - largest >= count - 1 else 0
    holding, rest = [largest] + [least] * (count - 1), total - largest - least * (count - 1)
    while rest > 0:
        free = [i for i in range(1, count) if holding[i] < largest] or [i for i in range(1, count) if holding[i] < most]
        whole, budget = sum([weights[i] for i in free]), rest
        for i in free:
            addition = min(most - holding[i], max(1, budget * weights[i] // whole), rest)
            holding[i] = holding[i] + addition
            rest = rest - addition
    return np.array(holding)


def gaussian(own_key, shape, deviation, most, shards=(), kind=jnp.bfloat16):
    values = deviation * jax.random.normal(own_key, shape, jnp.float32)
    if shards:
        values = values * level_of(own_key, shape, shards, -0.22, 0.18)
    return jnp.clip(values, -most, most).astype(kind)


def setup_inputs(seed: int = 0) -> dict:
    seeds = jax.random.split(jax.random.key(seed), 10)
    queries = draw_queries(jax.random.fold_in(seeds[9], 71), 0)
    projected_keys = draw_projected_keys(jax.random.fold_in(seeds[9], 71), 0)
    projected_values = gaussian(seeds[2], (SEQUENCE_TOKENS, KEY_VALUE_HEADS * HEAD_SIZE), 1.0, 6.0, ((0, 16), (1, 2)))
    hidden = gaussian(seeds[3], (SEQUENCE_TOKENS, D), 1.0, 6.0, ((0, 16), (1, 2)))
    route_ids_keys = jax.random.split(jax.random.fold_in(seeds[4], 1), SEQUENCE_TOKENS // TOK_DEV)
    route_ids_turns = jax.random.permutation(jax.random.fold_in(seeds[4], 3), SEQUENCE_TOKENS // TOK_DEV)
    route_ids = jax.vmap(lambda own, number: routed_block(jax.random.fold_in(seeds[4], 2), own, number, TOK_DEV, EXPERTS, 1, CAP, 2))(route_ids_keys, route_ids_turns).reshape((SEQUENCE_TOKENS, 1))
    route_gain = jnp.clip(0.25 + 0.75 * jax.random.uniform(seeds[5], (SEQUENCE_TOKENS,), jnp.float32) ** level_of(seeds[5], (SEQUENCE_TOKENS,), ((0, 16),), -0.2, 0.2), 0.25, 1.0)
    w_gate = gaussian(seeds[6], (EXPERTS * HOSTS, D, FF // HOSTS), D ** -0.5, 0.078125, ((0, 16), (2, 2)))
    w_up = gaussian(seeds[7], (EXPERTS * HOSTS, D, FF // HOSTS), D ** -0.5, 0.078125, ((0, 16), (2, 2)))
    w_down = gaussian(seeds[8], (EXPERTS * HOSTS, FF // HOSTS, D), FF ** -0.5, 0.09375, ((0, 16), (2, 2)))
    return dict(queries=queries, projected_keys=projected_keys, projected_values=projected_values, hidden=hidden, route_ids=route_ids, route_gain=route_gain, w_gate=w_gate, w_up=w_up, w_down=w_down)


def attend_all(queries, projected_keys, projected_values):
    head_group = QUERY_HEADS // KEY_VALUE_HEADS
    score_scale = HEAD_SIZE ** -0.5
    query_tensor = queries.reshape(SEQUENCE_TOKENS, KEY_VALUE_HEADS, head_group, HEAD_SIZE).astype(jnp.float32)
    key_tensor = projected_keys.reshape(SEQUENCE_TOKENS, KEY_VALUE_HEADS, HEAD_SIZE).astype(jnp.float32)
    value_tensor = projected_values.reshape(SEQUENCE_TOKENS, KEY_VALUE_HEADS, HEAD_SIZE).astype(jnp.float32)
    key_pos = jnp.arange(SEQUENCE_TOKENS, dtype=jnp.int32)
    block_rows = 512

    def one_block(block_index):
        query_part = lax.dynamic_slice_in_dim(query_tensor, (block_index * block_rows).astype(jnp.int32), block_rows, 0)
        query_pos = (block_index * block_rows + jnp.arange(block_rows, dtype=jnp.int32)).astype(jnp.int32)
        scores = jnp.einsum("qhgd,khd->hgqk", query_part, key_tensor) * score_scale
        allowed = query_pos[:, None] >= key_pos[None, :]
        scores = jnp.where(allowed, scores, -1e30)
        row_max = jnp.max(scores, axis=3, keepdims=True)
        weights = jnp.where(allowed, jnp.exp(scores - row_max), 0.0)
        denom = jnp.sum(weights, axis=3)
        rounded = lax.optimization_barrier(weights.astype(jnp.bfloat16)).astype(jnp.float32)
        result = jnp.einsum("hgqk,khd->qhgd", rounded, value_tensor)
        result = result / jnp.transpose(denom, (2, 0, 1))[..., None]
        return result.reshape(block_rows, QUERY_HEADS * HEAD_SIZE).astype(jnp.bfloat16)

    blocks = lax.map(one_block, jnp.arange(SEQUENCE_TOKENS // block_rows, dtype=jnp.int32))
    return blocks.reshape(SEQUENCE_TOKENS, QUERY_HEADS * HEAD_SIZE)


def experts_all(hidden, route_ids, route_gain, w_gate, w_up, w_down):
    host_count = N_CTX // EXPERTS
    share = FF // host_count
    ids_flat = route_ids[:, 0].astype(jnp.int32)
    chosen = (ids_flat[:, None] == jnp.arange(EXPERTS, dtype=jnp.int32)[None, :]).astype(jnp.int32)
    chosen = chosen.reshape(N_CTX, TOK_DEV, EXPERTS)
    ranking = jnp.sum((jnp.cumsum(chosen, axis=1) - chosen) * chosen, axis=2).reshape(SEQUENCE_TOKENS)
    source = jnp.arange(SEQUENCE_TOKENS, dtype=jnp.int32) // TOK_DEV
    slot_of = ((ids_flat * N_CTX + source) * CAP + ranking).astype(jnp.int32)
    table = jnp.zeros((EXPERTS * N_CTX * CAP, D), jnp.bfloat16).at[slot_of].set(hidden)
    table = table.reshape(EXPERTS, N_CTX * CAP, D)
    gate_grid = w_gate.reshape(EXPERTS, host_count, D, share)
    up_grid = w_up.reshape(EXPERTS, host_count, D, share)
    down_grid = w_down.reshape(EXPERTS, host_count, share, D)

    def one_expert(operands):
        rows_in, gate_w, up_w, down_w = operands
        inputs_f = rows_in.astype(jnp.float32)
        gate_val = jnp.einsum("rd,jdf->rjf", inputs_f, gate_w.astype(jnp.float32))
        up_val = jnp.einsum("rd,jdf->rjf", inputs_f, up_w.astype(jnp.float32))
        inner = lax.optimization_barrier((jax.nn.silu(gate_val) * up_val).astype(jnp.bfloat16)).astype(jnp.float32)
        partial_out = jnp.einsum("rjf,jfd->rjd", inner, down_w.astype(jnp.float32))
        partial_b = lax.optimization_barrier(partial_out.astype(jnp.bfloat16)).astype(jnp.float32)
        return jnp.sum(partial_b, axis=1)

    results = lax.map(one_expert, (table, gate_grid, up_grid, down_grid))
    results = results.reshape(EXPERTS * N_CTX * CAP, D)
    return (results[slot_of] * route_gain[:, None]).astype(jnp.bfloat16)


def reference(queries, projected_keys, projected_values, hidden, route_ids, route_gain, w_gate, w_up, w_down):
    attended = attend_all(queries, projected_keys, projected_values)
    mixed = experts_all(hidden, route_ids, route_gain, w_gate, w_up, w_down)
    return attended, mixed
```

```python
import functools
import math

import jax
import jax.numpy as jnp
from jax import lax
from jax.experimental import pallas as pl
from jax.experimental.pallas import tpu as pltpu
from jax.sharding import PartitionSpec as P


HEAD_SIZE = 128
EXPERTS = 16
CAP = 6

masked_score = -1e30
COVER = int(2e10)
sublane = 8
VMEM = pltpu.VMEM


def whole(n):
    return [pl.BlockSpec(memory_space=VMEM) for _ in range(n)]


def params(limit=8):
    return pltpu.CompilerParams(vmem_limit_bytes=limit * 1024 * 1024)


def far(array):
    return pltpu.with_memory_space_constraint(array, pltpu.HBM)


def near(*arrays):
    return [pltpu.with_memory_space_constraint(a, VMEM) for a in arrays]


def slots_of(ids_row):
    count = ids_row.shape[1]
    across = jnp.broadcast_to(ids_row, (count, count))
    down = across.T
    earlier = lax.broadcasted_iota(jnp.int32, (count, count), 0) < lax.broadcasted_iota(
        jnp.int32, (count, count), 1
    )
    same = jnp.where(jnp.logical_and(across == down, earlier), 1.0, 0.0)
    return jnp.sum(same, axis=0, keepdims=True)


def pack_kernel(place_ref, side_ref, ids_ref, hidden_hbm, key_hbm, value_hbm, packed_ref, kv_ref, hidden_ref, sems, *, pieces):
    width_kv = key_hbm.shape[1]
    copies = [
        pltpu.make_async_copy(hidden_hbm, hidden_ref, sems.at[0]),
        pltpu.make_async_copy(key_hbm, kv_ref.at[:, pl.ds(0, width_kv)], sems.at[1]),
        pltpu.make_async_copy(value_hbm, kv_ref.at[:, pl.ds(width_kv, width_kv)], sems.at[2]),
    ]
    for copy in copies:
        copy.start()
    ids_row = ids_ref[...].astype(jnp.float32)
    rank = slots_of(ids_row)
    rows = EXPERTS * CAP * pieces
    width = hidden_ref.shape[1] // pieces
    slot = ids_row * (CAP * pieces) + rank
    targets = jnp.concatenate([slot + float(k * CAP) for k in range(pieces)], axis=1)
    row_number = lax.broadcasted_iota(jnp.int32, (rows, targets.shape[1]), 0).astype(jnp.float32)
    selector = jnp.where(row_number == targets, 1.0, 0.0).astype(jnp.bfloat16)
    copies[0].wait()
    stacked = jnp.concatenate(
        [hidden_ref[:, k * width : (k + 1) * width] for k in range(pieces)], axis=0
    )
    out = jnp.dot(selector, stacked, preferred_element_type=jnp.float32).astype(jnp.bfloat16)
    packed_ref[...] = out.reshape(packed_ref.shape)
    copies[1].wait()
    copies[2].wait()


def pack(place, side, ids_row, hidden, keys, values, pieces):
    width = hidden.shape[1] // pieces
    return pl.pallas_call(
        functools.partial(pack_kernel, pieces=pieces),
        out_shape=(
            VMEM((EXPERTS, CAP * pieces, width), jnp.bfloat16),
            VMEM((keys.shape[0], 2 * keys.shape[1]), jnp.bfloat16),
        ),
        in_specs=[pl.BlockSpec(memory_space=pltpu.SMEM)] * 2
        + whole(1)
        + [pl.BlockSpec(memory_space=pl.ANY)] * 3,
        out_specs=tuple(whole(2)),
        scratch_shapes=[VMEM(hidden.shape, hidden.dtype), pltpu.SemaphoreType.DMA((3,))],
        compiler_params=params(4),
        cost_estimate=pl.CostEstimate(flops=COVER, bytes_accessed=1, transcendentals=0),
        name="pack",
    )(place, side, ids_row, far(hidden), far(keys), far(values))


def unpack_rows(arrived, pieces):
    rows, _ = arrived.shape
    per = rows // pieces
    group = CAP * pieces
    number = lax.broadcasted_iota(jnp.int32, (rows, 1), 0)
    piece, rest = number // per, number % per
    wanted = (rest // CAP) * group + piece * CAP + rest % CAP
    selector = jnp.where(
        lax.broadcasted_iota(jnp.int32, (rows, rows), 1) == wanted, 1.0, 0.0
    ).astype(jnp.bfloat16)
    out = jnp.dot(selector, arrived, preferred_element_type=jnp.float32).astype(jnp.bfloat16)
    return jnp.concatenate([out[k * per : (k + 1) * per] for k in range(pieces)], axis=1)


def column_blocks(width):
    wide = math.gcd(width, 512)
    return wide, width // wide


def halves(own, rest, side):
    return jnp.where(side == 0, own, rest), jnp.where(side == 0, rest, own)


def early_rows(w_down):
    return w_down.shape[1] * 3 // 4


def gate_up_kernel(side_ref, own_ref, rest_ref, wg_ref, wu_ref, wd_hbm, inner_ref, wd_ref, sems, *, pieces):
    early = wd_ref.shape[0]
    parts = sems.shape[0]
    copies = [
        pltpu.make_async_copy(
            wd_hbm.at[0, pl.ds(k * (early // parts), early // parts), :],
            wd_ref.at[pl.ds(k * (early // parts), early // parts), :],
            sems.at[k],
        )
        for k in range(parts)
    ]
    for copy in copies:
        copy.start()
    rows = own_ref.shape[0] * own_ref.shape[1]
    width = own_ref.shape[2]
    lo, hi = halves(own_ref[...].reshape(rows, width), rest_ref[...].reshape(rows, width), side_ref[0])
    x = jnp.concatenate([unpack_rows(lo, pieces), unpack_rows(hi, pieces)], axis=1)
    wide, blocks = column_blocks(wg_ref.shape[2])
    for n in range(blocks):
        at = slice(n * wide, (n + 1) * wide)
        gate = jnp.dot(x, wg_ref[0, :, at], preferred_element_type=jnp.float32)
        up = jnp.dot(x, wu_ref[0, :, at], preferred_element_type=jnp.float32)
        inner_ref[:, at] = (gate / (1.0 + jnp.exp(-gate)) * up).astype(jnp.bfloat16)
    for copy in copies:
        copy.wait()


def gate_up(side, own, rest, wg, wu, wd, pieces):
    rows = own.shape[0] * own.shape[1] // pieces
    near_spec = pl.BlockSpec(memory_space=VMEM)
    return pl.pallas_call(
        functools.partial(gate_up_kernel, pieces=pieces),
        out_shape=(
            VMEM((rows, wg.shape[2]), jnp.bfloat16),
            VMEM((early_rows(wd), wd.shape[2]), wd.dtype),
        ),
        in_specs=[pl.BlockSpec(memory_space=pltpu.SMEM)]
        + whole(4)
        + [pl.BlockSpec(memory_space=pl.ANY)],
        out_specs=(near_spec, near_spec),
        scratch_shapes=[pltpu.SemaphoreType.DMA((4,))],
        compiler_params=params(6),
        cost_estimate=pl.CostEstimate(
            flops=4 * rows * wg.size, bytes_accessed=wd.size, transcendentals=0
        ),
        name="gate_up",
    )(side, *near(own, rest, wg, wu), far(wd))


def down_kernel(side_ref, own_ref, rest_ref, wd_ref, wd_hbm, out_ref, buf, sem, *, pieces):
    early = wd_ref.shape[0]
    copy = pltpu.make_async_copy(wd_hbm.at[0, pl.ds(early, buf.shape[0]), :], buf, sem)
    copy.start()
    lo, hi = halves(own_ref[...], rest_ref[...], side_ref[0])
    x = jnp.concatenate([lo, hi], axis=1)
    per = x.shape[0]
    deep = math.gcd(early, buf.shape[0])
    wide, blocks = column_blocks(wd_ref.shape[1])

    def partial(ref, first, n, total):
        for k in range(ref.shape[0] // deep):
            rows = slice(k * deep, (k + 1) * deep)
            total = total + jnp.dot(
                x[:, first + k * deep : first + (k + 1) * deep],
                ref[rows, n * wide : (n + 1) * wide],
                preferred_element_type=jnp.float32,
            )
        return total

    zeros = jnp.zeros((per, wide), jnp.float32)
    totals = [partial(wd_ref, 0, n, zeros) for n in range(blocks)]
    copy.wait()
    full = jnp.concatenate(
        [partial(buf, early, n, totals[n]).astype(jnp.bfloat16) for n in range(blocks)], axis=1
    )
    width = full.shape[1] // pieces
    rounded = [full[:, k * width : (k + 1) * width] for k in range(pieces)]
    stacked = jnp.concatenate(rounded, axis=0)
    group = CAP * pieces
    rows = per * pieces
    number = lax.broadcasted_iota(jnp.int32, (rows, 1), 0)
    source, left = number // group, number % group
    wanted = (left // CAP) * per + source * CAP + left % CAP
    selector = jnp.where(
        lax.broadcasted_iota(jnp.int32, (rows, rows), 1) == wanted, 1.0, 0.0
    ).astype(jnp.bfloat16)
    out = jnp.dot(selector, stacked, preferred_element_type=jnp.float32).astype(jnp.bfloat16)
    out_ref[...] = out.reshape(out_ref.shape)


def down(side, own, rest, early, w, sources, pieces):
    left = w.shape[1] - early.shape[0]
    return pl.pallas_call(
        functools.partial(down_kernel, pieces=pieces),
        out_shape=VMEM((sources, CAP * pieces, w.shape[2] // pieces), jnp.bfloat16),
        in_specs=[pl.BlockSpec(memory_space=pltpu.SMEM)]
        + whole(3)
        + [pl.BlockSpec(memory_space=pl.ANY)],
        out_specs=pl.BlockSpec(memory_space=VMEM),
        scratch_shapes=[VMEM((left, w.shape[2]), w.dtype), pltpu.SemaphoreType.DMA],
        compiler_params=params(10),
        cost_estimate=pl.CostEstimate(
            flops=2 * own.shape[0] * w.size, bytes_accessed=w.size, transcendentals=0
        ),
        name="down",
    )(side, *near(own, rest, early), far(w))


def combine_kernel(ids_ref, gain_ref, back_ref, mixed_ref, *, pieces, hosts):
    ids_row = ids_ref[...].astype(jnp.float32)
    count = ids_row.shape[1]
    rank = slots_of(ids_row)
    width = back_ref.shape[3]
    group = CAP * pieces
    slot = ids_row * group + rank
    gain = jnp.broadcast_to(gain_ref[...], (sublane, count)).T[:, 0:1]
    first = jnp.broadcast_to(slot, (sublane, count)).T[:, 0:1]
    column = lax.broadcasted_iota(jnp.int32, (count, EXPERTS * group), 1).astype(jnp.float32)
    for k in range(pieces):
        selector = jnp.where(column == first + float(k * CAP), 1.0, 0.0).astype(jnp.bfloat16)
        picked = jnp.zeros((count, width), jnp.float32)
        for h in range(hosts):
            piece_rows = back_ref[h].reshape(EXPERTS * group, width)
            picked = picked + jnp.dot(selector, piece_rows, preferred_element_type=jnp.float32)
        mixed_ref[:, k * width : (k + 1) * width] = (picked * gain).astype(jnp.bfloat16)


def combine(ids_row, gain_row, back, pieces):
    hosts, _, _, width = back.shape
    return pl.pallas_call(
        functools.partial(combine_kernel, pieces=pieces, hosts=hosts),
        out_shape=jax.ShapeDtypeStruct((ids_row.shape[1], width * pieces), jnp.bfloat16),
        in_specs=whole(3),
        out_specs=pl.BlockSpec(memory_space=VMEM),
        compiler_params=params(),
        name="combine",
    )(*near(ids_row, gain_row, back))


def join_kernel(*refs):
    rows = refs[0].shape[0]
    for k, ref in enumerate(refs[:-1]):
        refs[-1][k * rows : (k + 1) * rows, :] = ref[...]


def join(parts):
    rows, width = parts[0].shape
    return pl.pallas_call(
        join_kernel,
        out_shape=VMEM((len(parts) * rows, width), parts[0].dtype),
        in_specs=whole(len(parts)),
        out_specs=pl.BlockSpec(memory_space=VMEM),
        compiler_params=params(),
        name="join",
    )(*near(*parts))


def attend_kernel(place_ref, query_ref, *refs, owner_of):
    out_ref = refs[-1]
    parts = refs[:-1]
    tok = query_ref.shape[0]
    kv_width = parts[0].shape[1] // 2
    kv_heads = kv_width // HEAD_SIZE
    group = query_ref.shape[1] // HEAD_SIZE // kv_heads
    me = place_ref[0]
    scale = HEAD_SIZE**-0.5
    rows = group * tok
    offset = lax.broadcasted_iota(jnp.int32, (rows, 1), 0)
    query_pos = me * tok + lax.rem(offset, tok)
    masks = []
    for p, part in enumerate(parts):
        count = part.shape[0]
        number = lax.broadcasted_iota(jnp.int32, (1, count), 1)
        block = lax.div(number, tok)
        owner, held = owner_of(me, p, block)
        key_pos = jnp.where(held, owner * tok + lax.rem(number, tok), jnp.iinfo(jnp.int32).max)
        masks.append(key_pos <= query_pos)
    for head in range(kv_heads):
        at = head * HEAD_SIZE
        first = head * group
        queries = jnp.concatenate(
            [
                query_ref[:, (first + g) * HEAD_SIZE : (first + g + 1) * HEAD_SIZE]
                for g in range(group)
            ],
            axis=0,
        )
        scores = []
        for part, mask in zip(parts, masks):
            score = lax.dot_general(
                queries,
                part[:, at : at + HEAD_SIZE],
                (((1,), (1,)), ((), ())),
                preferred_element_type=jnp.float32,
            )
            scores.append(jnp.where(mask, score * scale, masked_score))
        top = functools.reduce(jnp.maximum, [jnp.max(s, axis=1, keepdims=True) for s in scores])
        total = jnp.zeros((rows, 1), jnp.float32)
        mixed = jnp.zeros((rows, HEAD_SIZE), jnp.float32)
        for part, score in zip(parts, scores):
            weight = jnp.exp(score - top)
            total = total + jnp.sum(weight, axis=1, keepdims=True)
            mixed = mixed + jnp.dot(
                weight.astype(jnp.bfloat16),
                part[:, kv_width + at : kv_width + at + HEAD_SIZE],
                preferred_element_type=jnp.float32,
            )
        mixed = (mixed / total).astype(jnp.bfloat16)
        for g in range(group):
            out_ref[:, (first + g) * HEAD_SIZE : (first + g + 1) * HEAD_SIZE] = mixed[
                g * tok : (g + 1) * tok
            ]


def attend(place, queries, parts, owner_of):
    return pl.pallas_call(
        functools.partial(attend_kernel, owner_of=owner_of),
        out_shape=jax.ShapeDtypeStruct(queries.shape, jnp.bfloat16),
        in_specs=[pl.BlockSpec(memory_space=pltpu.SMEM)] + whole(1 + len(parts)),
        out_specs=pl.BlockSpec(memory_space=VMEM),
        compiler_params=params(8 + 40 * sum(p.shape[0] for p in parts) // 8192),
        name="attend",
    )(place, *near(queries, *parts))


plane = 4


def body(
    queries, projected_keys, projected_values, hidden, route_ids, route_gain, w_gate, w_up, w_down
):
    ctx_count = lax.axis_size("ctx")
    place = lax.axis_index("ctx").astype(jnp.int32).reshape(1)
    side = lax.axis_index("tp").astype(jnp.int32).reshape(1)
    hosts = ctx_count // EXPERTS
    pieces = sublane // math.gcd(CAP, sublane)
    ids_row = route_ids.reshape(1, -1)
    gain_row = route_gain.reshape(1, -1)

    packed, kv = pack(place, side, ids_row, hidden, projected_keys, projected_values, pieces)
    if hosts > 1:
        packed = jnp.repeat(packed, hosts, axis=0)
    arrived = lax.all_to_all(packed, "ctx", split_axis=0, concat_axis=0, tiled=True)

    if hosts == 1:
        slabs = [kv]
        for step in range(1, ctx_count // plane):
            pairs = [(i, i + step * plane) for i in range(ctx_count - step * plane)]
            slabs.append(lax.ppermute(kv, "ctx", pairs))
        column = join(slabs)
        parts = [column]
        for flip in range(1, plane):
            parts.append(lax.ppermute(column, "ctx", [(i, i ^ flip) for i in range(ctx_count)]))

        def owner_of(me, part, block):
            layer = lax.div(me, plane) - block
            return layer * plane + (lax.rem(me, plane) ^ part), layer >= 0
    else:
        parts = [lax.all_gather(kv, "ctx", axis=0, tiled=True)]

        def owner_of(me, part, block):
            return block, block >= 0

    other = [(0, 1), (1, 0)]
    arrived_rest = lax.ppermute(arrived, "tp", other)
    inner, early = gate_up(side, arrived, arrived_rest, w_gate, w_up, w_down, pieces)
    inner_rest = lax.ppermute(inner, "tp", other)
    result = down(side, inner, inner_rest, early, w_down, ctx_count, pieces)
    back = lax.all_to_all(result, "ctx", split_axis=0, concat_axis=0, tiled=True)
    attended = attend(place, queries, parts, owner_of)
    back = back.reshape(EXPERTS, hosts, CAP * pieces, -1).transpose(1, 0, 2, 3)
    mixed = combine(ids_row, gain_row, back, pieces)
    return (attended, mixed)


def general_body(
    queries, projected_keys, projected_values, hidden, route_ids, route_gain, w_gate, w_up, w_down
):
    tok_rows = queries.shape[0]
    width_q = queries.shape[1]
    width_kv = projected_keys.shape[1]
    ctx_count = lax.axis_size("ctx")
    ctx_index = lax.axis_index("ctx")
    offsets = jnp.arange(tok_rows, dtype=jnp.int32)
    query_use, key_use, value_use = (queries, projected_keys, projected_values)

    def position(device, offset):
        return device * tok_rows + offset

    query_pos = position(ctx_index, offsets)
    query_top = jnp.max(query_pos)
    kv_heads = width_kv // HEAD_SIZE
    head_group = width_q // HEAD_SIZE // kv_heads
    query_tensor = query_use.reshape(tok_rows, kv_heads, head_group, HEAD_SIZE)
    score_scale = HEAD_SIZE ** (-0.5)
    key_whole, value_whole = (
        lax.all_gather(key_use, "ctx", axis=0, tiled=True),
        lax.all_gather(value_use, "ctx", axis=0, tiled=True),
    )
    total_rows = key_whole.shape[0]
    block_rows = math.gcd(total_rows, 1024)

    def absorb_block(block_index, state):
        block_start = block_index * block_rows
        key_block = lax.dynamic_slice_in_dim(key_whole, block_start, block_rows, 0).reshape(
            block_rows, kv_heads, HEAD_SIZE
        )
        value_block = lax.dynamic_slice_in_dim(value_whole, block_start, block_rows, 0).reshape(
            block_rows, kv_heads, HEAD_SIZE
        )
        global_rows = block_start + jnp.arange(block_rows, dtype=jnp.int32)
        key_pos = position(global_rows // tok_rows, global_rows % tok_rows)

        def update(inner_state):
            running_max, running_sum, running_out = inner_state
            scores = (
                jnp.einsum(
                    "qhgd,khd->hgqk", query_tensor, key_block, preferred_element_type=jnp.float32
                )
                * score_scale
            )
            allowed = query_pos[:, None] >= key_pos[None, :]
            scores = jnp.where(allowed, scores, masked_score)
            new_max = jnp.maximum(running_max, jnp.max(scores, axis=3))
            weights = jnp.where(allowed, jnp.exp(scores - new_max[..., None]), 0.0)
            factor = jnp.exp(running_max - new_max)
            new_sum = running_sum * factor + jnp.sum(weights, axis=3)
            partial_out = jnp.einsum(
                "hgqk,khd->qhgd",
                weights.astype(jnp.bfloat16),
                value_block,
                preferred_element_type=jnp.float32,
            )
            new_out = running_out * jnp.transpose(factor, (2, 0, 1))[..., None] + partial_out
            return (new_max, new_sum, new_out)

        def keep_state(inner_state):
            return inner_state

        return lax.cond(jnp.min(key_pos) <= query_top, update, keep_state, state)

    initial = (
        jnp.full((kv_heads, head_group, tok_rows), masked_score, jnp.float32),
        jnp.zeros((kv_heads, head_group, tok_rows), jnp.float32),
        jnp.zeros((tok_rows, kv_heads, head_group, HEAD_SIZE), jnp.float32),
    )
    _, running_sum, running_out = lax.fori_loop(0, total_rows // block_rows, absorb_block, initial)
    attended = (
        (running_out / jnp.transpose(running_sum, (2, 0, 1))[..., None])
        .reshape(tok_rows, width_q)
        .astype(jnp.bfloat16)
    )
    ids_flat = route_ids[:, 0]
    chosen = (ids_flat[:, None] == jnp.arange(EXPERTS, dtype=jnp.int32)[None, :]).astype(jnp.int32)
    ranking = jnp.sum((jnp.cumsum(chosen, axis=0) - chosen) * chosen, axis=1)
    slot_of = ids_flat * CAP + ranking
    selector = (jnp.arange(EXPERTS * CAP, dtype=jnp.int32)[:, None] == slot_of[None, :]).astype(
        jnp.bfloat16
    )
    host_count = ctx_count // EXPERTS
    feature_width = hidden.shape[1]
    packed = jnp.dot(selector, hidden, preferred_element_type=jnp.float32).astype(jnp.bfloat16)
    packed = jnp.broadcast_to(
        packed.reshape(EXPERTS, 1, CAP, feature_width), (EXPERTS, host_count, CAP, feature_width)
    ).reshape(ctx_count, CAP, feature_width)
    arrived = lax.all_to_all(packed, "ctx", split_axis=0, concat_axis=0, tiled=True)
    arrived = lax.all_gather(arrived, "tp", axis=2, tiled=True)
    slot_count = arrived.shape[1]
    flat_rows = arrived.reshape(-1, arrived.shape[2])
    gate_val = jnp.dot(flat_rows, w_gate[0], preferred_element_type=jnp.float32)
    up_val = jnp.dot(flat_rows, w_up[0], preferred_element_type=jnp.float32)
    inner = (jax.nn.silu(gate_val) * up_val).astype(jnp.bfloat16)
    pair_inner = lax.all_gather(inner, "tp", axis=1, tiled=True)
    partial_out = jnp.dot(pair_inner, w_down[0], preferred_element_type=jnp.float32).astype(
        jnp.bfloat16
    )
    partial_out = partial_out.reshape(ctx_count, slot_count, partial_out.shape[1])
    returned = lax.all_to_all(partial_out, "ctx", split_axis=0, concat_axis=0, tiled=True)
    out_width = returned.shape[2]
    summed = returned.reshape(EXPERTS, host_count, CAP, out_width).astype(jnp.float32).sum(axis=1)
    summed = summed.reshape(EXPERTS * CAP, out_width)
    mixed = (summed[slot_of] * route_gain[:, None]).astype(jnp.bfloat16)
    return (attended, mixed)


def solution(mesh):
    in_specs = (
        P("ctx", "tp"),
        P("ctx", "tp"),
        P("ctx", "tp"),
        P("ctx", "tp"),
        P("ctx", None),
        P("ctx"),
        P("ctx", None, "tp"),
        P("ctx", None, "tp"),
        P("ctx", None, "tp"),
    )
    out_specs = (P("ctx", "tp"), P("ctx", "tp"))
    if mesh.shape["ctx"] != EXPERTS:
        return jax.shard_map(
            general_body, mesh=mesh, in_specs=in_specs, out_specs=out_specs, check_vma=False
        )
    return jax.shard_map(body, mesh=mesh, in_specs=in_specs, out_specs=out_specs, check_vma=False)
```

```python
import functools
import math

import jax
import jax.numpy as jnp
from jax import lax
from jax.experimental import pallas as pl
from jax.experimental.pallas import tpu as pltpu
from jax.sharding import PartitionSpec as P


HEAD_SIZE = 128
EXPERTS = 16
CAP = 6

masked_score = -1e30
COVER = int(2e10)
lane = 128
sublane = 8
VMEM = pltpu.VMEM


def whole(n):
    return [pl.BlockSpec(memory_space=VMEM) for _ in range(n)]


def params(limit=8):
    return pltpu.CompilerParams(vmem_limit_bytes=limit * 1024 * 1024)


def far(array):
    return pltpu.with_memory_space_constraint(array, pltpu.HBM)


def near(*arrays):
    return [pltpu.with_memory_space_constraint(a, VMEM) for a in arrays]


def slots_of(ids_row):
    count = ids_row.shape[1]
    across = jnp.broadcast_to(ids_row, (count, count))
    down = across.T
    earlier = lax.broadcasted_iota(jnp.int32, (count, count), 0) < lax.broadcasted_iota(
        jnp.int32, (count, count), 1
    )
    same = jnp.where(jnp.logical_and(across == down, earlier), 1.0, 0.0)
    return jnp.sum(same, axis=0, keepdims=True)


def pack_kernel(
    place_ref, side_ref, ids_hbm, hidden_hbm, key_hbm, value_hbm, packed_ref, kv_ref, ids_ref, hidden_ref, sems, *, pieces
):
    width_kv = key_hbm.shape[1]
    copies = [
        pltpu.make_async_copy(hidden_hbm, hidden_ref, sems.at[0]),
        pltpu.make_async_copy(key_hbm, kv_ref.at[:, pl.ds(0, width_kv)], sems.at[1]),
        pltpu.make_async_copy(value_hbm, kv_ref.at[:, pl.ds(width_kv, width_kv)], sems.at[2]),
    ]
    ids_copy = pltpu.make_async_copy(ids_hbm, ids_ref, sems.at[3])
    ids_copy.start()
    for copy in copies:
        copy.start()
    ids_copy.wait()
    ids_row = ids_ref[...].astype(jnp.float32)
    rank = slots_of(ids_row)
    rows = EXPERTS * CAP * pieces
    width = hidden_ref.shape[1] // pieces
    slot = ids_row * (CAP * pieces) + rank
    targets = jnp.concatenate([slot + float(k * CAP) for k in range(pieces)], axis=1)
    row_number = lax.broadcasted_iota(jnp.int32, (rows, targets.shape[1]), 0).astype(jnp.float32)
    selector = jnp.where(row_number == targets, 1.0, 0.0).astype(jnp.bfloat16)
    copies[0].wait()
    stacked = jnp.concatenate(
        [hidden_ref[:, k * width : (k + 1) * width] for k in range(pieces)], axis=0
    )
    out = jnp.dot(selector, stacked, preferred_element_type=jnp.float32).astype(jnp.bfloat16)
    packed_ref[...] = out.reshape(packed_ref.shape)
    copies[1].wait()
    copies[2].wait()


def pack(place, side, ids_row, hidden, keys, values, pieces):
    width = hidden.shape[1] // pieces
    return pl.pallas_call(
        functools.partial(pack_kernel, pieces=pieces),
        out_shape=(
            VMEM((EXPERTS, CAP * pieces, width), jnp.bfloat16),
            VMEM((keys.shape[0], 2 * keys.shape[1]), jnp.bfloat16),
        ),
        in_specs=[pl.BlockSpec(memory_space=pltpu.SMEM)] * 2
        + [pl.BlockSpec(memory_space=pl.ANY)] * 4,
        out_specs=tuple(whole(2)),
        scratch_shapes=[
            VMEM(ids_row.shape, ids_row.dtype),
            VMEM(hidden.shape, hidden.dtype),
            pltpu.SemaphoreType.DMA((4,)),
        ],
        compiler_params=params(4),
        cost_estimate=pl.CostEstimate(flops=COVER, bytes_accessed=1, transcendentals=0),
        name="pack",
    )(place, side, far(ids_row), far(hidden), far(keys), far(values))


def unpack_rows(arrived, pieces):
    rows, _ = arrived.shape
    per = rows // pieces
    group = CAP * pieces
    number = lax.broadcasted_iota(jnp.int32, (rows, 1), 0)
    piece, rest = number // per, number % per
    wanted = (rest // CAP) * group + piece * CAP + rest % CAP
    selector = jnp.where(
        lax.broadcasted_iota(jnp.int32, (rows, rows), 1) == wanted, 1.0, 0.0
    ).astype(jnp.bfloat16)
    out = jnp.dot(selector, arrived, preferred_element_type=jnp.float32).astype(jnp.bfloat16)
    return jnp.concatenate([out[k * per : (k + 1) * per] for k in range(pieces)], axis=1)


def column_blocks(width):
    wide = math.gcd(width, 512)
    return wide, width // wide


def early_rows(w_down):
    return w_down.shape[1] * 7 // 8


def gate_up_kernel(side_ref, own_ref, rest_ref, wg_ref, wu_ref, wd_hbm, inner_ref, wd_ref, x_ref, sems, *, pieces):
    side = side_ref[0]
    half = wd_hbm.shape[1] // 2
    early = wd_ref.shape[0]

    def fetch(k, place):
        from_row, to_row, count = ((place * half, 0, half), ((1 - place) * half, half, early - half))[k]
        return pltpu.make_async_copy(
            wd_hbm.at[0, pl.ds(from_row, count), :], wd_ref.at[pl.ds(to_row, count), :], sems.at[k]
        )

    for place in range(2):

        @pl.when(side == place)
        def _():
            for k in range(2):
                fetch(k, place).start()

    rows = own_ref.shape[0] * own_ref.shape[1]
    width = own_ref.shape[2]
    count = x_ref.shape[1] // 2
    for ref, place in ((own_ref, side), (rest_ref, 1 - side)):
        x_ref[:, pl.ds(pl.multiple_of(place * count, count), count)] = unpack_rows(
            ref[...].reshape(rows, width), pieces
        )
    x = x_ref[...]
    wide, blocks = column_blocks(wg_ref.shape[2])
    for n in range(blocks):
        at = slice(n * wide, (n + 1) * wide)
        gate = jnp.dot(x, wg_ref[0, :, at], preferred_element_type=jnp.float32)
        up = jnp.dot(x, wu_ref[0, :, at], preferred_element_type=jnp.float32)
        inner_ref[:, at] = (gate / (1.0 + jnp.exp(-gate)) * up).astype(jnp.bfloat16)
    for k in range(2):
        fetch(k, 0).wait()


def gate_up(side, own, rest, wg, wu, wd, pieces):
    rows = own.shape[0] * own.shape[1] // pieces
    near_spec = pl.BlockSpec(memory_space=VMEM)
    return pl.pallas_call(
        functools.partial(gate_up_kernel, pieces=pieces),
        out_shape=(
            VMEM((rows, wg.shape[2]), jnp.bfloat16),
            VMEM((early_rows(wd), wd.shape[2]), wd.dtype),
        ),
        in_specs=[pl.BlockSpec(memory_space=pltpu.SMEM)]
        + whole(4)
        + [pl.BlockSpec(memory_space=pl.ANY)],
        out_specs=(near_spec, near_spec),
        scratch_shapes=[
            VMEM((rows, wg.shape[1]), jnp.bfloat16),
            pltpu.SemaphoreType.DMA((2,)),
        ],
        compiler_params=params(4),
        cost_estimate=pl.CostEstimate(
            flops=4 * rows * wg.size, bytes_accessed=wd.size, transcendentals=0
        ),
        name="gate_up",
    )(side, *near(own, rest, wg, wu), far(wd))


def down_kernel(side_ref, own_ref, rest_ref, wd_ref, wd_hbm, out_ref, buf, acc_ref, stack_ref, sem, *, pieces):
    early = wd_ref.shape[0]
    half = wd_hbm.shape[1] // 2

    def fetch(place):
        at = (1 - place) * half + early - half
        return pltpu.make_async_copy(wd_hbm.at[0, pl.ds(at, buf.shape[0]), :], buf, sem)

    for place in range(2):

        @pl.when(side_ref[0] == place)
        def _():
            fetch(place).start()

    per = own_ref.shape[0]
    wide, blocks = column_blocks(wd_ref.shape[1])
    for n in range(blocks):
        at = slice(n * wide, (n + 1) * wide)
        acc_ref[:, at] = jnp.dot(
            own_ref[...], wd_ref[:half, at], preferred_element_type=jnp.float32
        ) + jnp.dot(
            rest_ref[:, : early - half], wd_ref[half:, at], preferred_element_type=jnp.float32
        )
    fetch(0).wait()
    width = stack_ref.shape[1]
    for n in range(blocks):
        at = slice(n * wide, (n + 1) * wide)
        total = acc_ref[:, at] + jnp.dot(
            rest_ref[:, early - half :], buf[:, at], preferred_element_type=jnp.float32
        )
        rounded = total.astype(jnp.bfloat16)
        for c in range(wide // lane):
            piece, column = divmod(n * wide + c * lane, width)
            stack_ref[piece * per : (piece + 1) * per, column : column + lane] = rounded[
                :, c * lane : (c + 1) * lane
            ]
    group = CAP * pieces
    rows = per * pieces
    number = lax.broadcasted_iota(jnp.int32, (rows, 1), 0)
    source, left = number // group, number % group
    wanted = (left // CAP) * per + source * CAP + left % CAP
    selector = jnp.where(
        lax.broadcasted_iota(jnp.int32, (rows, rows), 1) == wanted, 1.0, 0.0
    ).astype(jnp.bfloat16)
    out = jnp.dot(selector, stack_ref[...], preferred_element_type=jnp.float32).astype(jnp.bfloat16)
    out_ref[...] = out.reshape(out_ref.shape)


def down(side, own, rest, early, w, sources, pieces):
    left = w.shape[1] - early.shape[0]
    return pl.pallas_call(
        functools.partial(down_kernel, pieces=pieces),
        out_shape=VMEM((sources, CAP * pieces, w.shape[2] // pieces), jnp.bfloat16),
        in_specs=[pl.BlockSpec(memory_space=pltpu.SMEM)]
        + whole(3)
        + [pl.BlockSpec(memory_space=pl.ANY)],
        out_specs=pl.BlockSpec(memory_space=VMEM),
        scratch_shapes=[
            VMEM((left, w.shape[2]), w.dtype),
            VMEM((own.shape[0], w.shape[2]), jnp.float32),
            VMEM((own.shape[0] * pieces, w.shape[2] // pieces), jnp.bfloat16),
            pltpu.SemaphoreType.DMA,
        ],
        compiler_params=params(10),
        cost_estimate=pl.CostEstimate(
            flops=2 * own.shape[0] * w.size, bytes_accessed=w.size, transcendentals=0
        ),
        name="down",
    )(side, *near(own, rest, early), far(w))


def combine_kernel(ids_ref, gain_ref, back_ref, mixed_ref, *, pieces, hosts):
    ids_row = ids_ref[...].astype(jnp.float32)
    count = ids_row.shape[1]
    rank = slots_of(ids_row)
    width = back_ref.shape[3]
    group = CAP * pieces
    slot = ids_row * group + rank
    gain = jnp.broadcast_to(gain_ref[...], (sublane, count)).T[:, 0:1]
    first = jnp.broadcast_to(slot, (sublane, count)).T[:, 0:1]
    column = lax.broadcasted_iota(jnp.int32, (count, EXPERTS * group), 1).astype(jnp.float32)
    for k in range(pieces):
        selector = jnp.where(column == first + float(k * CAP), 1.0, 0.0).astype(jnp.bfloat16)
        picked = jnp.zeros((count, width), jnp.float32)
        for h in range(hosts):
            piece_rows = back_ref[h].reshape(EXPERTS * group, width)
            picked = picked + jnp.dot(selector, piece_rows, preferred_element_type=jnp.float32)
        mixed_ref[:, k * width : (k + 1) * width] = (picked * gain).astype(jnp.bfloat16)


def combine(ids_row, gain_row, back, pieces):
    hosts, _, _, width = back.shape
    return pl.pallas_call(
        functools.partial(combine_kernel, pieces=pieces, hosts=hosts),
        out_shape=jax.ShapeDtypeStruct((ids_row.shape[1], width * pieces), jnp.bfloat16),
        in_specs=whole(3),
        out_specs=pl.BlockSpec(memory_space=VMEM),
        compiler_params=params(),
        name="combine",
    )(*near(ids_row, gain_row, back))


def join_kernel(*refs, count):
    first = 0
    for ref in refs[:count]:
        refs[-1][first : first + ref.shape[0], :] = ref[...]
        first += ref.shape[0]


def join(parts, after=()):
    return pl.pallas_call(
        functools.partial(join_kernel, count=len(parts)),
        out_shape=VMEM((sum(p.shape[0] for p in parts), parts[0].shape[1]), parts[0].dtype),
        in_specs=whole(len(parts)) + [pl.BlockSpec(memory_space=pl.ANY)] * len(after),
        out_specs=pl.BlockSpec(memory_space=VMEM),
        compiler_params=params(2),
        name="join",
    )(*near(*parts), *after)


def attend_kernel(place_ref, query_ref, *refs, owner_of):
    out_ref = refs[-1]
    parts = refs[:-1]
    tok = query_ref.shape[0]
    kv_width = parts[0].shape[1] // 2
    kv_heads = kv_width // HEAD_SIZE
    group = query_ref.shape[1] // HEAD_SIZE // kv_heads
    me = place_ref[0]
    scale = HEAD_SIZE**-0.5
    rows = group * tok
    offset = lax.broadcasted_iota(jnp.int32, (rows, 1), 0)
    query_pos = me * tok + lax.rem(offset, tok)
    masks = []
    for p, part in enumerate(parts):
        count = part.shape[0]
        number = lax.broadcasted_iota(jnp.int32, (1, count), 1)
        block = lax.div(number, tok)
        owner, held = owner_of(me, p, block)
        key_pos = jnp.where(held, owner * tok + lax.rem(number, tok), jnp.iinfo(jnp.int32).max)
        masks.append(key_pos <= query_pos)
    for head in range(kv_heads):
        at = head * HEAD_SIZE
        first = head * group
        queries = jnp.concatenate(
            [
                query_ref[:, (first + g) * HEAD_SIZE : (first + g + 1) * HEAD_SIZE]
                for g in range(group)
            ],
            axis=0,
        )
        scores = []
        for part, mask in zip(parts, masks):
            score = lax.dot_general(
                queries,
                part[:, at : at + HEAD_SIZE],
                (((1,), (1,)), ((), ())),
                preferred_element_type=jnp.float32,
            )
            scores.append(jnp.where(mask, score * scale, masked_score))
        top = functools.reduce(jnp.maximum, [jnp.max(s, axis=1, keepdims=True) for s in scores])
        total = jnp.zeros((rows, 1), jnp.float32)
        mixed = jnp.zeros((rows, HEAD_SIZE), jnp.float32)
        for part, score in zip(parts, scores):
            weight = jnp.exp(score - top)
            total = total + jnp.sum(weight, axis=1, keepdims=True)
            mixed = mixed + jnp.dot(
                weight.astype(jnp.bfloat16),
                part[:, kv_width + at : kv_width + at + HEAD_SIZE],
                preferred_element_type=jnp.float32,
            )
        mixed = (mixed / total).astype(jnp.bfloat16)
        for g in range(group):
            out_ref[:, (first + g) * HEAD_SIZE : (first + g + 1) * HEAD_SIZE] = mixed[
                g * tok : (g + 1) * tok
            ]


def attend(place, queries, parts, owner_of):
    return pl.pallas_call(
        functools.partial(attend_kernel, owner_of=owner_of),
        out_shape=jax.ShapeDtypeStruct(queries.shape, jnp.bfloat16),
        in_specs=[pl.BlockSpec(memory_space=pltpu.SMEM)] + whole(1 + len(parts)),
        out_specs=pl.BlockSpec(memory_space=VMEM),
        compiler_params=params(8 + 40 * sum(p.shape[0] for p in parts) // 8192),
        name="attend",
    )(place, *near(queries, *parts))


plane = 4


def body(
    queries, projected_keys, projected_values, hidden, route_ids, route_gain, w_gate, w_up, w_down
):
    ctx_count = lax.axis_size("ctx")
    place = lax.axis_index("ctx").astype(jnp.int32).reshape(1)
    side = lax.axis_index("tp").astype(jnp.int32).reshape(1)
    hosts = ctx_count // EXPERTS
    pieces = sublane // math.gcd(CAP, sublane)
    ids_row = route_ids.reshape(1, -1)
    gain_row = route_gain.reshape(1, -1)

    packed, kv = pack(place, side, ids_row, hidden, projected_keys, projected_values, pieces)
    beside = lax.ppermute(kv, "ctx", [(i, i ^ plane) for i in range(ctx_count)])
    arrived = lax.all_to_all(packed, "ctx", split_axis=0, concat_axis=0, tiled=True)
    pair = join([kv, beside], (arrived,))
    below = lax.ppermute(pair, "ctx", [(i, i + 2 * plane) for i in range(ctx_count - 2 * plane)])
    column = join([pair, below])
    parts = [column]
    for flip in range(1, plane):
        parts.append(lax.ppermute(column, "ctx", [(i, i ^ flip) for i in range(ctx_count)]))

    def owner_of(me, part, block):
        layer = lax.div(me, plane)
        held = jnp.logical_or(block < 2, layer >= 2)
        return (layer ^ block) * plane + (lax.rem(me, plane) ^ part), held

    other = [(0, 1), (1, 0)]
    arrived_rest = lax.ppermute(arrived, "tp", other)
    inner, early = gate_up(side, arrived, arrived_rest, w_gate, w_up, w_down, pieces)
    inner_rest = lax.ppermute(inner, "tp", other)
    result = down(side, inner, inner_rest, early, w_down, ctx_count, pieces)
    back = lax.all_to_all(result, "ctx", split_axis=0, concat_axis=0, tiled=True)
    attended = attend(place, queries, parts, owner_of)
    back = back.reshape(EXPERTS, hosts, CAP * pieces, -1).transpose(1, 0, 2, 3)
    mixed = combine(ids_row, gain_row, back, pieces)
    return (attended, mixed)


def general_body(
    queries, projected_keys, projected_values, hidden, route_ids, route_gain, w_gate, w_up, w_down
):
    tok_rows = queries.shape[0]
    width_q = queries.shape[1]
    width_kv = projected_keys.shape[1]
    ctx_count = lax.axis_size("ctx")
    ctx_index = lax.axis_index("ctx")
    offsets = jnp.arange(tok_rows, dtype=jnp.int32)
    query_use, key_use, value_use = (queries, projected_keys, projected_values)

    def position(device, offset):
        return device * tok_rows + offset

    query_pos = position(ctx_index, offsets)
    query_top = jnp.max(query_pos)
    kv_heads = width_kv // HEAD_SIZE
    head_group = width_q // HEAD_SIZE // kv_heads
    query_tensor = query_use.reshape(tok_rows, kv_heads, head_group, HEAD_SIZE)
    score_scale = HEAD_SIZE ** (-0.5)
    key_whole, value_whole = (
        lax.all_gather(key_use, "ctx", axis=0, tiled=True),
        lax.all_gather(value_use, "ctx", axis=0, tiled=True),
    )
    total_rows = key_whole.shape[0]
    block_rows = math.gcd(total_rows, 1024)

    def absorb_block(block_index, state):
        block_start = block_index * block_rows
        key_block = lax.dynamic_slice_in_dim(key_whole, block_start, block_rows, 0).reshape(
            block_rows, kv_heads, HEAD_SIZE
        )
        value_block = lax.dynamic_slice_in_dim(value_whole, block_start, block_rows, 0).reshape(
            block_rows, kv_heads, HEAD_SIZE
        )
        global_rows = block_start + jnp.arange(block_rows, dtype=jnp.int32)
        key_pos = position(global_rows // tok_rows, global_rows % tok_rows)

        def update(inner_state):
            running_max, running_sum, running_out = inner_state
            scores = (
                jnp.einsum(
                    "qhgd,khd->hgqk", query_tensor, key_block, preferred_element_type=jnp.float32
                )
                * score_scale
            )
            allowed = query_pos[:, None] >= key_pos[None, :]
            scores = jnp.where(allowed, scores, masked_score)
            new_max = jnp.maximum(running_max, jnp.max(scores, axis=3))
            weights = jnp.where(allowed, jnp.exp(scores - new_max[..., None]), 0.0)
            factor = jnp.exp(running_max - new_max)
            new_sum = running_sum * factor + jnp.sum(weights, axis=3)
            partial_out = jnp.einsum(
                "hgqk,khd->qhgd",
                weights.astype(jnp.bfloat16),
                value_block,
                preferred_element_type=jnp.float32,
            )
            new_out = running_out * jnp.transpose(factor, (2, 0, 1))[..., None] + partial_out
            return (new_max, new_sum, new_out)

        def keep_state(inner_state):
            return inner_state

        return lax.cond(jnp.min(key_pos) <= query_top, update, keep_state, state)

    initial = (
        jnp.full((kv_heads, head_group, tok_rows), masked_score, jnp.float32),
        jnp.zeros((kv_heads, head_group, tok_rows), jnp.float32),
        jnp.zeros((tok_rows, kv_heads, head_group, HEAD_SIZE), jnp.float32),
    )
    _, running_sum, running_out = lax.fori_loop(0, total_rows // block_rows, absorb_block, initial)
    attended = (
        (running_out / jnp.transpose(running_sum, (2, 0, 1))[..., None])
        .reshape(tok_rows, width_q)
        .astype(jnp.bfloat16)
    )
    ids_flat = route_ids[:, 0]
    chosen = (ids_flat[:, None] == jnp.arange(EXPERTS, dtype=jnp.int32)[None, :]).astype(jnp.int32)
    ranking = jnp.sum((jnp.cumsum(chosen, axis=0) - chosen) * chosen, axis=1)
    slot_of = ids_flat * CAP + ranking
    selector = (jnp.arange(EXPERTS * CAP, dtype=jnp.int32)[:, None] == slot_of[None, :]).astype(
        jnp.bfloat16
    )
    host_count = ctx_count // EXPERTS
    feature_width = hidden.shape[1]
    packed = jnp.dot(selector, hidden, preferred_element_type=jnp.float32).astype(jnp.bfloat16)
    packed = jnp.broadcast_to(
        packed.reshape(EXPERTS, 1, CAP, feature_width), (EXPERTS, host_count, CAP, feature_width)
    ).reshape(ctx_count, CAP, feature_width)
    arrived = lax.all_to_all(packed, "ctx", split_axis=0, concat_axis=0, tiled=True)
    arrived = lax.all_gather(arrived, "tp", axis=2, tiled=True)
    slot_count = arrived.shape[1]
    flat_rows = arrived.reshape(-1, arrived.shape[2])
    gate_val = jnp.dot(flat_rows, w_gate[0], preferred_element_type=jnp.float32)
    up_val = jnp.dot(flat_rows, w_up[0], preferred_element_type=jnp.float32)
    inner = (jax.nn.silu(gate_val) * up_val).astype(jnp.bfloat16)
    pair_inner = lax.all_gather(inner, "tp", axis=1, tiled=True)
    partial_out = jnp.dot(pair_inner, w_down[0], preferred_element_type=jnp.float32).astype(
        jnp.bfloat16
    )
    partial_out = partial_out.reshape(ctx_count, slot_count, partial_out.shape[1])
    returned = lax.all_to_all(partial_out, "ctx", split_axis=0, concat_axis=0, tiled=True)
    out_width = returned.shape[2]
    summed = returned.reshape(EXPERTS, host_count, CAP, out_width).astype(jnp.float32).sum(axis=1)
    summed = summed.reshape(EXPERTS * CAP, out_width)
    mixed = (summed[slot_of] * route_gain[:, None]).astype(jnp.bfloat16)
    return (attended, mixed)


def solution(mesh):
    in_specs = (
        P("ctx", "tp"),
        P("ctx", "tp"),
        P("ctx", "tp"),
        P("ctx", "tp"),
        P("ctx", None),
        P("ctx"),
        P("ctx", None, "tp"),
        P("ctx", None, "tp"),
        P("ctx", None, "tp"),
    )
    out_specs = (P("ctx", "tp"), P("ctx", "tp"))
    if mesh.shape["ctx"] != EXPERTS:
        return jax.shard_map(
            general_body, mesh=mesh, in_specs=in_specs, out_specs=out_specs, check_vma=False
        )
    return jax.shard_map(body, mesh=mesh, in_specs=in_specs, out_specs=out_specs, check_vma=False)
```

```python
import functools
import math

import jax
import jax.numpy as jnp
from jax import lax
from jax.experimental import pallas as pl
from jax.experimental.pallas import tpu as pltpu
from jax.sharding import PartitionSpec as P


HEAD_SIZE = 128
EXPERTS = 16
CAP = 6

masked_score = -1e30
COVER = int(2e10)
lane = 128
sublane = 8
VMEM = pltpu.VMEM


def whole(n):
    return [pl.BlockSpec(memory_space=VMEM) for _ in range(n)]


def params(limit=8):
    return pltpu.CompilerParams(vmem_limit_bytes=limit * 1024 * 1024)


def far(array):
    return pltpu.with_memory_space_constraint(array, pltpu.HBM)


def near(*arrays):
    return [pltpu.with_memory_space_constraint(a, VMEM) for a in arrays]


def slots_of(ids_row):
    count = ids_row.shape[1]
    across = jnp.broadcast_to(ids_row, (count, count))
    down = across.T
    earlier = lax.broadcasted_iota(jnp.int32, (count, count), 0) < lax.broadcasted_iota(
        jnp.int32, (count, count), 1
    )
    same = jnp.where(jnp.logical_and(across == down, earlier), 1.0, 0.0)
    return jnp.sum(same, axis=0, keepdims=True)


def pack_kernel(
    place_ref, side_ref, ids_hbm, hidden_hbm, key_hbm, value_hbm, packed_ref, kv_ref, ids_ref, hidden_ref, sems, *, pieces
):
    width_kv = key_hbm.shape[1]
    copies = [
        pltpu.make_async_copy(hidden_hbm, hidden_ref, sems.at[0]),
        pltpu.make_async_copy(key_hbm, kv_ref.at[:, pl.ds(0, width_kv)], sems.at[1]),
        pltpu.make_async_copy(value_hbm, kv_ref.at[:, pl.ds(width_kv, width_kv)], sems.at[2]),
    ]
    ids_copy = pltpu.make_async_copy(ids_hbm, ids_ref, sems.at[3])
    ids_copy.start()
    for copy in copies:
        copy.start()
    ids_copy.wait()
    ids_row = ids_ref[...].astype(jnp.float32)
    rank = slots_of(ids_row)
    rows = EXPERTS * CAP * pieces
    width = hidden_ref.shape[1] // pieces
    slot = ids_row * (CAP * pieces) + rank
    targets = jnp.concatenate([slot + float(k * CAP) for k in range(pieces)], axis=1)
    row_number = lax.broadcasted_iota(jnp.int32, (rows, targets.shape[1]), 0).astype(jnp.float32)
    selector = jnp.where(row_number == targets, 1.0, 0.0).astype(jnp.bfloat16)
    copies[0].wait()
    stacked = jnp.concatenate(
        [hidden_ref[:, k * width : (k + 1) * width] for k in range(pieces)], axis=0
    )
    out = jnp.dot(selector, stacked, preferred_element_type=jnp.float32).astype(jnp.bfloat16)
    packed_ref[...] = out.reshape(packed_ref.shape)
    copies[1].wait()
    copies[2].wait()


def pack(place, side, ids_row, hidden, keys, values, pieces):
    width = hidden.shape[1] // pieces
    return pl.pallas_call(
        functools.partial(pack_kernel, pieces=pieces),
        out_shape=(
            VMEM((EXPERTS, CAP * pieces, width), jnp.bfloat16),
            VMEM((keys.shape[0], 2 * keys.shape[1]), jnp.bfloat16),
        ),
        in_specs=[pl.BlockSpec(memory_space=pltpu.SMEM)] * 2
        + [pl.BlockSpec(memory_space=pl.ANY)] * 4,
        out_specs=tuple(whole(2)),
        scratch_shapes=[
            VMEM(ids_row.shape, ids_row.dtype),
            VMEM(hidden.shape, hidden.dtype),
            pltpu.SemaphoreType.DMA((4,)),
        ],
        compiler_params=params(4),
        cost_estimate=pl.CostEstimate(flops=COVER, bytes_accessed=1, transcendentals=0),
        name="pack",
    )(place, side, far(ids_row), far(hidden), far(keys), far(values))


def unpack_rows(arrived, pieces):
    rows, _ = arrived.shape
    per = rows // pieces
    group = CAP * pieces
    number = lax.broadcasted_iota(jnp.int32, (rows, 1), 0)
    piece, rest = number // per, number % per
    wanted = (rest // CAP) * group + piece * CAP + rest % CAP
    selector = jnp.where(
        lax.broadcasted_iota(jnp.int32, (rows, rows), 1) == wanted, 1.0, 0.0
    ).astype(jnp.bfloat16)
    out = jnp.dot(selector, arrived, preferred_element_type=jnp.float32).astype(jnp.bfloat16)
    return jnp.concatenate([out[k * per : (k + 1) * per] for k in range(pieces)], axis=1)


def column_blocks(width):
    wide = math.gcd(width, 512)
    return wide, width // wide


def early_rows(w_down):
    return w_down.shape[1] * 7 // 8


def gate_up_kernel(side_ref, own_ref, rest_ref, wg_ref, wu_ref, wd_hbm, inner_ref, wd_ref, x_ref, sems, *, pieces):
    side = side_ref[0]
    half = wd_hbm.shape[1] // 2
    early = wd_ref.shape[0]

    def fetch(k, place):
        from_row, to_row, count = ((place * half, 0, half), ((1 - place) * half, half, early - half))[k]
        return pltpu.make_async_copy(
            wd_hbm.at[0, pl.ds(from_row, count), :], wd_ref.at[pl.ds(to_row, count), :], sems.at[k]
        )

    for place in range(2):

        @pl.when(side == place)
        def _():
            for k in range(2):
                fetch(k, place).start()

    rows = own_ref.shape[0] * own_ref.shape[1]
    width = own_ref.shape[2]
    count = x_ref.shape[1] // 2
    for ref, place in ((own_ref, side), (rest_ref, 1 - side)):
        x_ref[:, pl.ds(pl.multiple_of(place * count, count), count)] = unpack_rows(
            ref[...].reshape(rows, width), pieces
        )
    x = x_ref[...]
    wide, blocks = column_blocks(wg_ref.shape[2])
    for n in range(blocks):
        at = slice(n * wide, (n + 1) * wide)
        gate = jnp.dot(x, wg_ref[0, :, at], preferred_element_type=jnp.float32)
        up = jnp.dot(x, wu_ref[0, :, at], preferred_element_type=jnp.float32)
        inner_ref[:, at] = (gate / (1.0 + jnp.exp(-gate)) * up).astype(jnp.bfloat16)
    for k in range(2):
        fetch(k, 0).wait()


def gate_up(side, own, rest, wg, wu, wd, pieces):
    rows = own.shape[0] * own.shape[1] // pieces
    near_spec = pl.BlockSpec(memory_space=VMEM)
    return pl.pallas_call(
        functools.partial(gate_up_kernel, pieces=pieces),
        out_shape=(
            VMEM((rows, wg.shape[2]), jnp.bfloat16),
            VMEM((early_rows(wd), wd.shape[2]), wd.dtype),
        ),
        in_specs=[pl.BlockSpec(memory_space=pltpu.SMEM)]
        + whole(4)
        + [pl.BlockSpec(memory_space=pl.ANY)],
        out_specs=(near_spec, near_spec),
        scratch_shapes=[
            VMEM((rows, wg.shape[1]), jnp.bfloat16),
            pltpu.SemaphoreType.DMA((2,)),
        ],
        compiler_params=params(4),
        cost_estimate=pl.CostEstimate(
            flops=4 * rows * wg.size, bytes_accessed=wd.size, transcendentals=0
        ),
        name="gate_up",
    )(side, *near(own, rest, wg, wu), far(wd))


def down_kernel(
    side_ref, own_ref, rest_ref, wd_ref, wd_hbm, out_hbm, out_ref, buf, acc_ref, stack_ref, sem, out_sems, *, pieces
):
    early = wd_ref.shape[0]
    half = wd_hbm.shape[1] // 2

    def fetch(place):
        at = (1 - place) * half + early - half
        return pltpu.make_async_copy(wd_hbm.at[0, pl.ds(at, buf.shape[0]), :], buf, sem)

    for place in range(2):

        @pl.when(side_ref[0] == place)
        def _():
            fetch(place).start()

    per = own_ref.shape[0]
    wide, blocks = column_blocks(wd_ref.shape[1])
    for n in range(blocks):
        at = slice(n * wide, (n + 1) * wide)
        acc_ref[:, at] = jnp.dot(
            own_ref[...], wd_ref[:half, at], preferred_element_type=jnp.float32
        ) + jnp.dot(
            rest_ref[:, : early - half], wd_ref[half:, at], preferred_element_type=jnp.float32
        )
    fetch(0).wait()
    width = stack_ref.shape[1]
    for n in range(blocks):
        at = slice(n * wide, (n + 1) * wide)
        total = acc_ref[:, at] + jnp.dot(
            rest_ref[:, early - half :], buf[:, at], preferred_element_type=jnp.float32
        )
        rounded = total.astype(jnp.bfloat16)
        for c in range(wide // lane):
            piece, column = divmod(n * wide + c * lane, width)
            stack_ref[piece * per : (piece + 1) * per, column : column + lane] = rounded[
                :, c * lane : (c + 1) * lane
            ]
    group = CAP * pieces
    rows = per * pieces
    number = lax.broadcasted_iota(jnp.int32, (rows, 1), 0)
    source, left = number // group, number % group
    wanted = (left // CAP) * per + source * CAP + left % CAP
    parts = out_sems.shape[0]
    count = rows // parts
    sources = out_hbm.shape[0] // parts
    copies = []
    for p in range(parts):
        at = slice(p * count, (p + 1) * count)
        selector = jnp.where(
            lax.broadcasted_iota(jnp.int32, (count, rows), 1) == wanted[at], 1.0, 0.0
        ).astype(jnp.bfloat16)
        out = jnp.dot(selector, stack_ref[...], preferred_element_type=jnp.float32)
        blocks_at = slice(p * sources, (p + 1) * sources)
        out_ref[blocks_at] = out.astype(jnp.bfloat16).reshape((sources,) + out_ref.shape[1:])
        copies.append(
            pltpu.make_async_copy(out_ref.at[blocks_at], out_hbm.at[blocks_at], out_sems.at[p])
        )
        copies[-1].start()
    for done in copies:
        done.wait()


def down(side, own, rest, early, w, sources, pieces):
    left = w.shape[1] - early.shape[0]
    return pl.pallas_call(
        functools.partial(down_kernel, pieces=pieces),
        out_shape=pltpu.HBM((sources, CAP * pieces, w.shape[2] // pieces), jnp.bfloat16),
        in_specs=[pl.BlockSpec(memory_space=pltpu.SMEM)]
        + whole(3)
        + [pl.BlockSpec(memory_space=pl.ANY)],
        out_specs=pl.BlockSpec(memory_space=pl.ANY),
        scratch_shapes=[
            VMEM((sources, CAP * pieces, w.shape[2] // pieces), jnp.bfloat16),
            VMEM((left, w.shape[2]), w.dtype),
            VMEM((own.shape[0], w.shape[2]), jnp.float32),
            VMEM((own.shape[0] * pieces, w.shape[2] // pieces), jnp.bfloat16),
            pltpu.SemaphoreType.DMA,
            pltpu.SemaphoreType.DMA((2,)),
        ],
        compiler_params=params(10),
        cost_estimate=pl.CostEstimate(
            flops=2 * own.shape[0] * w.size, bytes_accessed=w.size, transcendentals=0
        ),
        name="down",
    )(side, *near(own, rest, early), far(w))


def route_columns(ids_ref, gain_ref, route_ref, pieces):
    ids_row = ids_ref[...].astype(jnp.float32)
    slot = ids_row * (CAP * pieces) + slots_of(ids_row)
    route_ref[:, :lane] = jnp.broadcast_to(slot, (lane, slot.shape[1])).T
    route_ref[:, lane:] = jnp.broadcast_to(gain_ref[...], (lane, slot.shape[1])).T


def combine_kernel(route_ref, back_ref, mixed_hbm, mixed_ref, sems, *, pieces):
    count = route_ref.shape[0]
    experts, group, width = back_ref.shape
    back = back_ref[...].reshape(experts * group, width)
    slot = route_ref[:, 0:1]
    gain = route_ref[:, lane : lane + 1]
    column = lax.broadcasted_iota(jnp.int32, (count, experts * group), 1).astype(jnp.float32)
    copies = []
    for k in range(pieces):
        selector = jnp.where(column == slot + float(k * CAP), 1.0, 0.0).astype(jnp.bfloat16)
        picked = jnp.dot(selector, back, preferred_element_type=jnp.float32)
        at = slice(k * width, (k + 1) * width)
        mixed_ref[:, at] = (picked * gain).astype(jnp.bfloat16)
        copies.append(pltpu.make_async_copy(mixed_ref.at[:, at], mixed_hbm.at[:, at], sems.at[k]))
        copies[-1].start()
    for copy in copies:
        copy.wait()


def combine(route, back, pieces):
    count, width = route.shape[0], back.shape[2] * pieces
    return pl.pallas_call(
        functools.partial(combine_kernel, pieces=pieces),
        out_shape=pltpu.HBM((count, width), jnp.bfloat16),
        in_specs=whole(2),
        out_specs=pl.BlockSpec(memory_space=pl.ANY),
        scratch_shapes=[
            VMEM((count, width), jnp.bfloat16),
            pltpu.SemaphoreType.DMA((pieces,)),
        ],
        compiler_params=params(4),
        name="combine",
    )(*near(route, back))


def join_kernel(*refs, count):
    first = 0
    for ref in refs[:count]:
        refs[-1][first : first + ref.shape[0], :] = ref[...]
        first += ref.shape[0]


def join(parts, after=()):
    return pl.pallas_call(
        functools.partial(join_kernel, count=len(parts)),
        out_shape=VMEM((sum(p.shape[0] for p in parts), parts[0].shape[1]), parts[0].dtype),
        in_specs=whole(len(parts)) + [pl.BlockSpec(memory_space=pl.ANY)] * len(after),
        out_specs=pl.BlockSpec(memory_space=VMEM),
        compiler_params=params(2),
        name="join",
    )(*near(*parts), *after)


def attend_kernel(place_ref, ids_ref, gain_ref, query_ref, *refs, owner_of, pieces):
    out_ref, route_ref = refs[-2:]
    parts = refs[:-2]
    route_columns(ids_ref, gain_ref, route_ref, pieces)
    tok = query_ref.shape[0]
    kv_width = parts[0].shape[1] // 2
    kv_heads = kv_width // HEAD_SIZE
    group = query_ref.shape[1] // HEAD_SIZE // kv_heads
    me = place_ref[0]
    scale = HEAD_SIZE**-0.5
    rows = group * tok
    offset = lax.broadcasted_iota(jnp.int32, (rows, 1), 0)
    query_pos = me * tok + lax.rem(offset, tok)
    masks = []
    for p, part in enumerate(parts):
        count = part.shape[0]
        number = lax.broadcasted_iota(jnp.int32, (1, count), 1)
        block = lax.div(number, tok)
        owner, held = owner_of(me, p, block)
        key_pos = jnp.where(held, owner * tok + lax.rem(number, tok), jnp.iinfo(jnp.int32).max)
        masks.append(key_pos <= query_pos)
    for head in range(kv_heads):
        at = head * HEAD_SIZE
        first = head * group
        queries = jnp.concatenate(
            [
                query_ref[:, (first + g) * HEAD_SIZE : (first + g + 1) * HEAD_SIZE]
                for g in range(group)
            ],
            axis=0,
        )
        scores = []
        for part, mask in zip(parts, masks):
            score = lax.dot_general(
                queries,
                part[:, at : at + HEAD_SIZE],
                (((1,), (1,)), ((), ())),
                preferred_element_type=jnp.float32,
            )
            scores.append(jnp.where(mask, score * scale, masked_score))
        top = functools.reduce(jnp.maximum, [jnp.max(s, axis=1, keepdims=True) for s in scores])
        total = jnp.zeros((rows, 1), jnp.float32)
        mixed = jnp.zeros((rows, HEAD_SIZE), jnp.float32)
        for part, score in zip(parts, scores):
            weight = jnp.exp(score - top)
            total = total + jnp.sum(weight, axis=1, keepdims=True)
            mixed = mixed + jnp.dot(
                weight.astype(jnp.bfloat16),
                part[:, kv_width + at : kv_width + at + HEAD_SIZE],
                preferred_element_type=jnp.float32,
            )
        mixed = (mixed / total).astype(jnp.bfloat16)
        for g in range(group):
            out_ref[:, (first + g) * HEAD_SIZE : (first + g + 1) * HEAD_SIZE] = mixed[
                g * tok : (g + 1) * tok
            ]


def attend(place, ids_row, gain_row, queries, parts, owner_of, pieces):
    return pl.pallas_call(
        functools.partial(attend_kernel, owner_of=owner_of, pieces=pieces),
        out_shape=(
            jax.ShapeDtypeStruct(queries.shape, jnp.bfloat16),
            VMEM((queries.shape[0], 2 * lane), jnp.float32),
        ),
        in_specs=[pl.BlockSpec(memory_space=pltpu.SMEM)] + whole(3 + len(parts)),
        out_specs=tuple(whole(2)),
        compiler_params=params(8 + 40 * sum(p.shape[0] for p in parts) // 8192),
        name="attend",
    )(place, *near(ids_row, gain_row, queries, *parts))


plane = 4


def body(
    queries, projected_keys, projected_values, hidden, route_ids, route_gain, w_gate, w_up, w_down
):
    ctx_count = lax.axis_size("ctx")
    place = lax.axis_index("ctx").astype(jnp.int32).reshape(1)
    side = lax.axis_index("tp").astype(jnp.int32).reshape(1)
    pieces = sublane // math.gcd(CAP, sublane)
    ids_row = route_ids.reshape(1, -1)
    gain_row = route_gain.reshape(1, -1)

    packed, kv = pack(place, side, ids_row, hidden, projected_keys, projected_values, pieces)
    beside = lax.ppermute(kv, "ctx", [(i, i ^ plane) for i in range(ctx_count)])
    arrived = lax.all_to_all(packed, "ctx", split_axis=0, concat_axis=0, tiled=True)
    pair = join([kv, beside], (arrived,))
    below = lax.ppermute(pair, "ctx", [(i, i + 2 * plane) for i in range(ctx_count - 2 * plane)])
    column = join([pair, below])
    parts = [column]
    for flip in range(1, plane):
        parts.append(lax.ppermute(column, "ctx", [(i, i ^ flip) for i in range(ctx_count)]))

    def owner_of(me, part, block):
        layer = lax.div(me, plane)
        held = jnp.logical_or(block < 2, layer >= 2)
        return (layer ^ block) * plane + (lax.rem(me, plane) ^ part), held

    other = [(0, 1), (1, 0)]
    arrived_rest = lax.ppermute(arrived, "tp", other)
    inner, early = gate_up(side, arrived, arrived_rest, w_gate, w_up, w_down, pieces)
    inner_rest = lax.ppermute(inner, "tp", other)
    result = down(side, inner, inner_rest, early, w_down, ctx_count, pieces)
    back = lax.all_to_all(result, "ctx", split_axis=0, concat_axis=0, tiled=True)
    attended, route = attend(place, ids_row, gain_row, queries, parts, owner_of, pieces)
    mixed = combine(route, back, pieces)
    return (attended, mixed)


def general_body(
    queries, projected_keys, projected_values, hidden, route_ids, route_gain, w_gate, w_up, w_down
):
    tok_rows = queries.shape[0]
    width_q = queries.shape[1]
    width_kv = projected_keys.shape[1]
    ctx_count = lax.axis_size("ctx")
    ctx_index = lax.axis_index("ctx")
    offsets = jnp.arange(tok_rows, dtype=jnp.int32)
    query_use, key_use, value_use = (queries, projected_keys, projected_values)

    def position(device, offset):
        return device * tok_rows + offset

    query_pos = position(ctx_index, offsets)
    query_top = jnp.max(query_pos)
    kv_heads = width_kv // HEAD_SIZE
    head_group = width_q // HEAD_SIZE // kv_heads
    query_tensor = query_use.reshape(tok_rows, kv_heads, head_group, HEAD_SIZE)
    score_scale = HEAD_SIZE ** (-0.5)
    key_whole, value_whole = (
        lax.all_gather(key_use, "ctx", axis=0, tiled=True),
        lax.all_gather(value_use, "ctx", axis=0, tiled=True),
    )
    total_rows = key_whole.shape[0]
    block_rows = math.gcd(total_rows, 1024)

    def absorb_block(block_index, state):
        block_start = block_index * block_rows
        key_block = lax.dynamic_slice_in_dim(key_whole, block_start, block_rows, 0).reshape(
            block_rows, kv_heads, HEAD_SIZE
        )
        value_block = lax.dynamic_slice_in_dim(value_whole, block_start, block_rows, 0).reshape(
            block_rows, kv_heads, HEAD_SIZE
        )
        global_rows = block_start + jnp.arange(block_rows, dtype=jnp.int32)
        key_pos = position(global_rows // tok_rows, global_rows % tok_rows)

        def update(inner_state):
            running_max, running_sum, running_out = inner_state
            scores = (
                jnp.einsum(
                    "qhgd,khd->hgqk", query_tensor, key_block, preferred_element_type=jnp.float32
                )
                * score_scale
            )
            allowed = query_pos[:, None] >= key_pos[None, :]
            scores = jnp.where(allowed, scores, masked_score)
            new_max = jnp.maximum(running_max, jnp.max(scores, axis=3))
            weights = jnp.where(allowed, jnp.exp(scores - new_max[..., None]), 0.0)
            factor = jnp.exp(running_max - new_max)
            new_sum = running_sum * factor + jnp.sum(weights, axis=3)
            partial_out = jnp.einsum(
                "hgqk,khd->qhgd",
                weights.astype(jnp.bfloat16),
                value_block,
                preferred_element_type=jnp.float32,
            )
            new_out = running_out * jnp.transpose(factor, (2, 0, 1))[..., None] + partial_out
            return (new_max, new_sum, new_out)

        def keep_state(inner_state):
            return inner_state

        return lax.cond(jnp.min(key_pos) <= query_top, update, keep_state, state)

    initial = (
        jnp.full((kv_heads, head_group, tok_rows), masked_score, jnp.float32),
        jnp.zeros((kv_heads, head_group, tok_rows), jnp.float32),
        jnp.zeros((tok_rows, kv_heads, head_group, HEAD_SIZE), jnp.float32),
    )
    _, running_sum, running_out = lax.fori_loop(0, total_rows // block_rows, absorb_block, initial)
    attended = (
        (running_out / jnp.transpose(running_sum, (2, 0, 1))[..., None])
        .reshape(tok_rows, width_q)
        .astype(jnp.bfloat16)
    )
    ids_flat = route_ids[:, 0]
    chosen = (ids_flat[:, None] == jnp.arange(EXPERTS, dtype=jnp.int32)[None, :]).astype(jnp.int32)
    ranking = jnp.sum((jnp.cumsum(chosen, axis=0) - chosen) * chosen, axis=1)
    slot_of = ids_flat * CAP + ranking
    selector = (jnp.arange(EXPERTS * CAP, dtype=jnp.int32)[:, None] == slot_of[None, :]).astype(
        jnp.bfloat16
    )
    host_count = ctx_count // EXPERTS
    feature_width = hidden.shape[1]
    packed = jnp.dot(selector, hidden, preferred_element_type=jnp.float32).astype(jnp.bfloat16)
    packed = jnp.broadcast_to(
        packed.reshape(EXPERTS, 1, CAP, feature_width), (EXPERTS, host_count, CAP, feature_width)
    ).reshape(ctx_count, CAP, feature_width)
    arrived = lax.all_to_all(packed, "ctx", split_axis=0, concat_axis=0, tiled=True)
    arrived = lax.all_gather(arrived, "tp", axis=2, tiled=True)
    slot_count = arrived.shape[1]
    flat_rows = arrived.reshape(-1, arrived.shape[2])
    gate_val = jnp.dot(flat_rows, w_gate[0], preferred_element_type=jnp.float32)
    up_val = jnp.dot(flat_rows, w_up[0], preferred_element_type=jnp.float32)
    inner = (jax.nn.silu(gate_val) * up_val).astype(jnp.bfloat16)
    pair_inner = lax.all_gather(inner, "tp", axis=1, tiled=True)
    partial_out = jnp.dot(pair_inner, w_down[0], preferred_element_type=jnp.float32).astype(
        jnp.bfloat16
    )
    partial_out = partial_out.reshape(ctx_count, slot_count, partial_out.shape[1])
    returned = lax.all_to_all(partial_out, "ctx", split_axis=0, concat_axis=0, tiled=True)
    out_width = returned.shape[2]
    summed = returned.reshape(EXPERTS, host_count, CAP, out_width).astype(jnp.float32).sum(axis=1)
    summed = summed.reshape(EXPERTS * CAP, out_width)
    mixed = (summed[slot_of] * route_gain[:, None]).astype(jnp.bfloat16)
    return (attended, mixed)


def solution(mesh):
    in_specs = (
        P("ctx", "tp"),
        P("ctx", "tp"),
        P("ctx", "tp"),
        P("ctx", "tp"),
        P("ctx", None),
        P("ctx"),
        P("ctx", None, "tp"),
        P("ctx", None, "tp"),
        P("ctx", None, "tp"),
    )
    out_specs = (P("ctx", "tp"), P("ctx", "tp"))
    if mesh.shape["ctx"] != EXPERTS:
        return jax.shard_map(
            general_body, mesh=mesh, in_specs=in_specs, out_specs=out_specs, check_vma=False
        )
    return jax.shard_map(body, mesh=mesh, in_specs=in_specs, out_specs=out_specs, check_vma=False)
```
